32 devices in a mesh: dp: 4 (over y, z), tp: 8 (over x, core).
Axes of the slice: x: 4, y: 2, z: 2, core: 2. Of those that a mesh axis runs over, the one named last changes fastest.
The devices are a block of a 4x4x8 slice.
Arguments:
- x_chunk: bfloat16 [16, 1024, 2048], P('dp', 'tp'), parts along dimension 0
- prefix_len: int32 [16], P('dp'), parts along dimension 0
- k_cache: bfloat16 [16, 4096, 16, 128], P('dp', None, 'tp'), parts along dimension 0
- v_cache: bfloat16 [16, 4096, 16, 128], P('dp', None, 'tp'), parts along dimension 0
- ln1_gain: bfloat16 [2048], replicated
- ln1_bias: bfloat16 [2048], replicated
- w_qkv: bfloat16 [2048, 6144], P(None, 'tp')
- b_qkv: bfloat16 [6144], P('tp')
- w_out: bfloat16 [2048, 2048], P('tp')
- b_out: bfloat16 [2048], replicated
- ln2_gain: bfloat16 [2048], replicated
- ln2_bias: bfloat16 [2048], replicated
- w_up: bfloat16 [2048, 8192], P(None, 'tp')
- b_up: bfloat16 [8192], P('tp')
- w_down: bfloat16 [8192, 2048], P('tp')
- b_down: bfloat16 [2048], replicated
Outputs:
- output 1: bfloat16 [16, 1024, 2048], P('dp', 'tp'), parts along dimension 0
- output 2: bfloat16 [16, 4096, 16, 128], P('dp', None, 'tp'), parts along dimension 0
- output 3: bfloat16 [16, 4096, 16, 128], P('dp', None, 'tp'), parts along dimension 0
There are 4 independent parts. The reference program is written for one: setup_inputs(seed, part) draws one part's arguments, and reference() takes and returns one part's arrays. A program takes and returns all parts, laid end to end along the dimension named above; an argument that names none is the same for every part.
All inputs are finite; a program needn't handle non-finite values.
Results may differ from the reference program's by a relative error of at most 0.0132017.
Values are sent between devices in bfloat16 or wider.
A program may use at most 768 MiB of HBM per device.

```python
import jax
import jax.numpy as jnp
from jax import lax

BATCH_SEQS = 4
CHUNK_LEN = 1024
CACHE_LEN = 4096
D_MODEL = 2048
NUM_HEADS = 16
HEAD_DIM = 128
FF_DIM = 4 * D_MODEL
LN_EPS = 1e-5


def setup_inputs(seed: int = 0, part: int = 0) -> dict:
    part_keys = jax.random.split(jax.random.fold_in(jax.random.key(seed), part), 5)
    shared_keys = jax.random.split(jax.random.key(seed + 7919), 12)
    max_start = CACHE_LEN - CHUNK_LEN
    starts = jax.random.randint(part_keys[1], (BATCH_SEQS,), 0, max_start + 1)
    longest = jax.random.randint(part_keys[2], (), 0, BATCH_SEQS)
    prefix_len = jnp.where(jnp.arange(BATCH_SEQS) == longest, max_start, starts).astype(jnp.int32)
    cache_shape = (BATCH_SEQS, CACHE_LEN, NUM_HEADS, HEAD_DIM)
    vec_shape = (D_MODEL,)
    d_scale = D_MODEL ** -0.5

    def normal_draw(key_in, shape_in, std_dev):
        return (std_dev * jax.random.normal(key_in, shape_in, jnp.float32)).astype(jnp.bfloat16)

    def gain_draw(key_in):
        return (1.0 + 0.25 * jax.random.normal(key_in, vec_shape, jnp.float32)).astype(jnp.bfloat16)

    return {
        'x_chunk': normal_draw(part_keys[0], (BATCH_SEQS, CHUNK_LEN, D_MODEL), 1.0),
        'prefix_len': prefix_len,
        'k_cache': normal_draw(part_keys[3], cache_shape, 1.0),
        'v_cache': normal_draw(part_keys[4], cache_shape, 1.0),
        'ln1_gain': gain_draw(shared_keys[0]),
        'ln1_bias': normal_draw(shared_keys[1], vec_shape, 0.25),
        'w_qkv': normal_draw(shared_keys[2], (D_MODEL, 3 * D_MODEL), d_scale),
        'b_qkv': normal_draw(shared_keys[3], (3 * D_MODEL,), 0.25),
        'w_out': normal_draw(shared_keys[4], (D_MODEL, D_MODEL), d_scale),
        'b_out': normal_draw(shared_keys[5], vec_shape, 0.25),
        'ln2_gain': gain_draw(shared_keys[6]),
        'ln2_bias': normal_draw(shared_keys[7], vec_shape, 0.25),
        'w_up': normal_draw(shared_keys[8], (D_MODEL, FF_DIM), d_scale),
        'b_up': normal_draw(shared_keys[9], (FF_DIM,), 0.25),
        'w_down': normal_draw(shared_keys[10], (FF_DIM, D_MODEL), FF_DIM ** -0.5),
        'b_down': normal_draw(shared_keys[11], vec_shape, 0.25),
    }


def layer_norm(tok_rows, ln_gain, ln_bias):
    rows_f32 = tok_rows.astype(jnp.float32)
    row_mean = jnp.mean(rows_f32, axis=-1, keepdims=True)
    centered = rows_f32 - row_mean
    row_var = jnp.mean(centered * centered, axis=-1, keepdims=True)
    normed = centered * lax.rsqrt(row_var + LN_EPS)
    return (normed * ln_gain.astype(jnp.float32) + ln_bias.astype(jnp.float32)).astype(jnp.bfloat16)


def write_rows(cache_seq, new_rows, start_pos):
    zero_idx = jnp.zeros_like(start_pos)
    return lax.dynamic_update_slice(cache_seq, new_rows, (start_pos, zero_idx, zero_idx))


def attend_one(operands):
    queries, keys_all, values_all, start_pos = operands
    scores = jnp.einsum('chd,thd->hct', queries.astype(jnp.float32), keys_all.astype(jnp.float32)) * (HEAD_DIM ** -0.5)
    slopes = jnp.exp2(-8.0 * (jnp.arange(NUM_HEADS) + 1).astype(jnp.float32) / NUM_HEADS)
    query_pos = start_pos + jnp.arange(CHUNK_LEN)
    rel_pos = (jnp.arange(CACHE_LEN)[None, :] - query_pos[:, None]).astype(jnp.float32)
    scores = scores + slopes[:, None, None] * rel_pos[None]
    scores = jnp.where((rel_pos <= 0.0)[None], scores, -1e30)
    attn_probs = jax.nn.softmax(scores, axis=-1).astype(jnp.bfloat16)
    context = jnp.einsum('hct,thd->chd', attn_probs.astype(jnp.float32), values_all.astype(jnp.float32))
    return context.astype(jnp.bfloat16).reshape(CHUNK_LEN, D_MODEL)


def reference(x_chunk, prefix_len, k_cache, v_cache, ln1_gain, ln1_bias, w_qkv, b_qkv, w_out, b_out, ln2_gain, ln2_bias, w_up, b_up, w_down, b_down):
    tok_rows = x_chunk.reshape(BATCH_SEQS * CHUNK_LEN, D_MODEL)
    normed = layer_norm(tok_rows, ln1_gain, ln1_bias)
    qkv_proj = jnp.dot(normed, w_qkv, preferred_element_type=jnp.float32) + b_qkv.astype(jnp.float32)
    qkv_heads = qkv_proj.astype(jnp.bfloat16).reshape(BATCH_SEQS, CHUNK_LEN, NUM_HEADS, 3, HEAD_DIM)
    k_upd = jax.vmap(write_rows)(k_cache, qkv_heads[:, :, :, 1], prefix_len)
    v_upd = jax.vmap(write_rows)(v_cache, qkv_heads[:, :, :, 2], prefix_len)
    context = lax.map(attend_one, (qkv_heads[:, :, :, 0], k_upd, v_upd, prefix_len))
    context = context.reshape(BATCH_SEQS * CHUNK_LEN, D_MODEL)
    attn_out = jnp.dot(context, w_out, preferred_element_type=jnp.float32)
    residual = (tok_rows.astype(jnp.float32) + attn_out + b_out.astype(jnp.float32)).astype(jnp.bfloat16)
    normed2 = layer_norm(residual, ln2_gain, ln2_bias)
    up_pre = jnp.dot(normed2, w_up, preferred_element_type=jnp.float32) + b_up.astype(jnp.float32)
    up_act = jax.nn.gelu(up_pre, approximate=True).astype(jnp.bfloat16)
    down_out = jnp.dot(up_act, w_down, preferred_element_type=jnp.float32)
    x_out = (residual.astype(jnp.float32) + down_out + b_down.astype(jnp.float32)).astype(jnp.bfloat16)
    return x_out.reshape(BATCH_SEQS, CHUNK_LEN, D_MODEL), k_upd, v_upd
```

```python
import functools
import math

import jax
import jax.numpy as jnp
from jax import lax
from jax.experimental import pallas as pl
from jax.experimental.pallas import tpu as pltpu
from jax.sharding import PartitionSpec as P


LN_EPS = 1e-5
LOG2E = math.log2(math.e)
NEG = -1e30


def layer_norm(tok_rows, ln_gain, ln_bias):
    rows_f32 = tok_rows.astype(jnp.float32)
    row_mean = jnp.mean(rows_f32, axis=-1, keepdims=True)
    centered = rows_f32 - row_mean
    row_var = jnp.mean(centered * centered, axis=-1, keepdims=True)
    normed = centered * lax.rsqrt(row_var + LN_EPS)
    return (normed * ln_gain.astype(jnp.float32) + ln_bias.astype(jnp.float32)).astype(jnp.bfloat16)


def attn_kernel(seq, q_blk, k_blk, prefix_ref, slope_ref, qkv_ref, k_ref, v_ref, *rest):
    out_ref, knew_ref, vnew_ref, acc_ref, m_ref = rest[-5:]
    head = pl.program_id(0)
    chunk = qkv_ref.shape[0]
    dim = k_ref.shape[3]
    heads = qkv_ref.shape[1] // (3 * dim)
    start = prefix_ref[seq]
    slope = slope_ref[head] * LOG2E
    scale = dim ** -0.5 * LOG2E

    def ones(n):
        return (lax.broadcasted_iota(jnp.int32, (n, dim), 1) == 0).astype(jnp.bfloat16)

    def cols(which):
        return pl.ds(pl.multiple_of((3 * head + which) * dim, dim), dim)

    @pl.when(head == 0)
    def _():
        n = 256
        row = lax.broadcasted_iota(jnp.int32, (n, n), 0)
        pick = (row // heads + row % heads * (n // heads) == lax.broadcasted_iota(jnp.int32, (n, n), 1)).astype(jnp.bfloat16)
        for which, dst in ((1, knew_ref), (2, vnew_ref)):
            for i in range(heads * chunk // n):
                rows = pl.ds(i * (n // heads), n // heads)
                both = jnp.concatenate([qkv_ref[rows, (3 * h + which) * dim:(3 * h + which + 1) * dim] for h in range(heads)], axis=0)
                dst[pl.ds(i * n, n), :] = jnp.dot(pick, both, preferred_element_type=jnp.float32).astype(dst.dtype)

    def update(rows, keys, values, bias, masked=None):
        s = lax.dot_general(qkv_ref[rows, cols(0)], keys, (((1,), (1,)), ((), ())), preferred_element_type=jnp.float32)
        s = s * scale + bias
        if masked is not None:
            s = jnp.where(masked, NEG, s)
        m_old = m_ref[rows, :1]
        m_new = jnp.maximum(m_old, jnp.max(s, axis=1, keepdims=True))
        p = jnp.exp2(s - m_new).astype(jnp.bfloat16)
        pv = lax.dot_general(p, jnp.concatenate([values, ones(values.shape[0])], axis=1), (((1,), (0,)), ((), ())), preferred_element_type=jnp.float32)
        acc_ref[rows, :] = acc_ref[rows, :] * jnp.exp2(m_old - m_new) + pv
        m_ref[rows, :] = jnp.broadcast_to(m_new, (q_blk, m_ref.shape[1]))

    col = lax.broadcasted_iota(jnp.int32, (1, k_blk), 1)
    acc_ref[...] = jnp.zeros_like(acc_ref)
    m_ref[...] = jnp.full_like(m_ref, NEG)
    full = start // k_blk

    def prefix_block(i, masked):
        off = pl.multiple_of(i * k_blk, k_blk)
        keys = k_ref[0, 0, pl.ds(off, k_blk), :]
        values = v_ref[0, 0, pl.ds(off, k_blk), :]
        rel = (off + col - start).astype(jnp.float32)
        for r in range(chunk // q_blk):
            update(pl.ds(r * q_blk, q_blk), keys, values, slope * (rel - float(r * q_blk)), (off + col >= start) if masked else None)

    @pl.loop(0, full)
    def _(i):
        prefix_block(i, False)

    @pl.when(full * k_blk < start)
    def _():
        prefix_block(full, True)

    for r in range(chunk // q_blk):
        n = (r + 1) * q_blk
        new_col = lax.broadcasted_iota(jnp.int32, (1, n), 1) - r * q_blk
        bias = slope * new_col.astype(jnp.float32)
        masked = (lax.broadcasted_iota(jnp.int32, (q_blk, n), 1) - r * q_blk) > lax.broadcasted_iota(jnp.int32, (q_blk, n), 0)
        update(pl.ds(r * q_blk, q_blk), qkv_ref[pl.ds(0, n), cols(1)], qkv_ref[pl.ds(0, n), cols(2)], bias, masked)
    total = acc_ref[:, dim:dim + 1]
    out_ref[:, 0] = (acc_ref[:, :dim] / total).astype(out_ref.dtype).reshape(out_ref.shape[0], out_ref.shape[2], dim)


def attend(seq, prefix_len, slopes, qkv, k_heads, v_heads, owners=8, slots=1, slot=0, buffer=None, q_blk=256, k_blk=1024):
    chunk = qkv.shape[0]
    heads, cache_len, dim = k_heads.shape[1:]
    cache_spec = pl.BlockSpec((1, 1, cache_len, dim), lambda h, *_: (seq, h, 0, 0))
    whole = lambda shape: pl.BlockSpec(shape, lambda h, *_: (0, 0))
    rows = jax.ShapeDtypeStruct((heads * chunk, dim), jnp.bfloat16)
    extra = () if buffer is None else (buffer,)
    return pl.pallas_call(
        functools.partial(attn_kernel, seq, q_blk, k_blk),
        out_shape=(jax.ShapeDtypeStruct((owners, slots, chunk // owners, heads * dim), jnp.bfloat16), rows, rows),
        grid_spec=pltpu.PrefetchScalarGridSpec(
            num_scalar_prefetch=2,
            grid=(heads,),
            in_specs=[whole(qkv.shape), cache_spec, cache_spec] + [pl.BlockSpec(memory_space=pl.ANY)] * len(extra),
            out_specs=(pl.BlockSpec((owners, 1, chunk // owners, dim), lambda h, *_: (0, slot, 0, h)), whole(rows.shape), whole(rows.shape)),
            scratch_shapes=[pltpu.VMEM((chunk, 2 * dim), jnp.float32), pltpu.VMEM((chunk, 128), jnp.float32)],
        ),
        cost_estimate=pl.CostEstimate(flops=4 * heads * chunk * cache_len * dim, bytes_accessed=4 * heads * cache_len * dim, transcendentals=heads * chunk * cache_len),
        input_output_aliases={5: 0} if extra else {},
        name='attend',
    )(prefix_len, slopes, qkv, k_heads, v_heads, *extra)


def prep_kernel(heads, event_ref, k_ref, v_ref, k_copy, v_copy, k_heads, v_heads):
    del event_ref
    n = 256
    per = n // heads
    row = lax.broadcasted_iota(jnp.int32, (n, n), 0)
    pick = (row % per * heads + row // per == lax.broadcasted_iota(jnp.int32, (n, n), 1)).astype(jnp.bfloat16)
    for src, copy, split in ((k_ref, k_copy, k_heads), (v_ref, v_copy, v_heads)):
        copy[...] = src[...]
        for i in range(src.shape[1] // n):
            both = jnp.dot(pick, src[0, pl.ds(i * n, n), :], preferred_element_type=jnp.float32).astype(split.dtype)
            for h in range(heads):
                split[0, h, pl.ds(i * per, per), :] = both[h * per:(h + 1) * per]


def prep_cache(k_cache, v_cache, event, rows=2048):
    batch, length, heads, dim = k_cache.shape
    flat = (batch, length * heads, dim)
    flat_spec = pl.BlockSpec((1, rows, dim), lambda b, i: (b, i, 0))
    split_spec = pl.BlockSpec((1, heads, rows // heads, dim), lambda b, i: (b, 0, i, 0))
    flat_out = jax.ShapeDtypeStruct(flat, k_cache.dtype)
    split_out = jax.ShapeDtypeStruct((batch, heads, length, dim), k_cache.dtype)
    k_copy, v_copy, k_heads, v_heads = pl.pallas_call(
        functools.partial(prep_kernel, heads),
        out_shape=(flat_out, flat_out, split_out, split_out),
        grid=(batch, length * heads // rows),
        in_specs=[pl.BlockSpec(memory_space=pl.ANY), flat_spec, flat_spec],
        out_specs=(flat_spec, flat_spec, split_spec, split_spec),
        cost_estimate=pl.CostEstimate(flops=8 * batch * length * heads * dim * 256, bytes_accessed=12 * batch * length * heads * dim, transcendentals=0),
        name='prep',
    )(event, k_cache.reshape(flat), v_cache.reshape(flat))
    return k_copy.reshape(k_cache.shape), v_copy.reshape(k_cache.shape), k_heads, v_heads


def proj_kernel(early_ref, late_ref, x_ref, w_ref, b_ref, gain_ref, bias_ref, res_ref, norm_ref, owned, wide):
    step = pl.program_id(0)
    blocks, early, tok, part = early_ref.shape
    batch = x_ref.shape[0]

    @pl.when(step == 0)
    def _():
        for b in range(batch):
            src, at = (early_ref, b) if b < early else (late_ref, b - early)
            for t in range(blocks):
                owned[b * tok:(b + 1) * tok, t * part:(t + 1) * part] = src[t, at]

    tile = w_ref.shape[1]
    total = jnp.dot(owned[...], w_ref[...], preferred_element_type=jnp.float32)
    for b in range(batch):
        row = (x_ref[b].astype(jnp.float32) + total[b * tok:(b + 1) * tok] + b_ref[...]).astype(res_ref.dtype)
        res_ref[b] = row
        wide[b * tok:(b + 1) * tok, pl.ds(pl.multiple_of(step * tile, tile), tile)] = row

    @pl.when(step == pl.num_programs(0) - 1)
    def _():
        n = 64

        @pl.loop(0, wide.shape[0] // n)
        def _(i):
            rows = pl.ds(pl.multiple_of(i * n, n), n)
            val = wide[rows, :].astype(jnp.float32)
            centered = val - jnp.mean(val, axis=-1, keepdims=True)
            var = jnp.mean(centered * centered, axis=-1, keepdims=True)
            norm_ref[rows, :] = (centered * lax.rsqrt(var + LN_EPS) * gain_ref[...] + bias_ref[...]).astype(norm_ref.dtype)


def project(early, late, x, w, b, gain, bias, tile=512):
    batch, tok, width = x.shape
    whole = lambda a: pl.BlockSpec(a.shape, lambda j: (0,) * a.ndim)
    row = lambda a: a.astype(jnp.float32)[None]
    gain, bias = row(gain), row(bias)
    bf16 = jnp.bfloat16
    col = pl.BlockSpec((batch, tok, tile), lambda j: (0, 0, j))
    return pl.pallas_call(
        proj_kernel,
        out_shape=(jax.ShapeDtypeStruct(x.shape, bf16), jax.ShapeDtypeStruct((batch * tok, width), bf16)),
        grid=(width // tile,),
        in_specs=[whole(early), whole(late), col, pl.BlockSpec((width, tile), lambda j: (0, j)), pl.BlockSpec((1, tile), lambda j: (0, j)), whole(gain), whole(bias)],
        out_specs=(col, pl.BlockSpec((batch * tok, width), lambda j: (0, 0))),
        scratch_shapes=[pltpu.VMEM((batch * tok, width), bf16), pltpu.VMEM((batch * tok, width), bf16)],
        cost_estimate=pl.CostEstimate(flops=2 * batch * tok * width * width, bytes_accessed=2 * width * width, transcendentals=0),
        name='project',
    )(early, late, x, w, row(b), gain, bias)


def pair_ids(t):
    return {'mate': t + 1 - 2 * (t % 2), 'partner': t + 2 - 4 * (t // 2 % 2)}


def mlp_kernel(a_ref, res_ref, wu_ref, wd_ref, u0, u1, u2, u3, d0, d1, d2, d3, bu_ref, bd_ref, out_ref,
               wu, wd, rows, hid, stage, own, to_mate, to_diag, to_partner, from_mate, from_diag, from_partner, res,
               load_sem, send_sem, recv_sem):
    me = lax.axis_index('tp')
    ids = pair_ids(me)
    quarter = lax.axis_index('dp') % 4
    q_1 = quarter + 1 - 2 * (quarter % 2)
    q_2 = quarter + 2 - 4 * (quarter // 2)
    q_3 = 3 - quarter
    tok, width = own.shape
    blk = hid.shape[0]
    halves = tok // blk
    hid_loc = wu.shape[2]
    tile = 512

    barrier = pltpu.get_barrier_semaphore()
    for who in ('mate', 'partner'):
        pl.semaphore_signal(barrier, inc=1, device_id={'tp': ids[who]}, device_id_type=pl.DeviceIdType.MESH)

    loads = [pltpu.make_async_copy(a_ref, rows.at[0], load_sem.at[0]), pltpu.make_async_copy(wu_ref, wu.at[0], load_sem.at[1])]
    q_rows = u0.shape[0]
    for i, (piece, at) in enumerate(((u0, quarter), (u1, q_1), (u2, q_2), (u3, q_3))):
        loads.append(pltpu.make_async_copy(piece, wu.at[1, pl.ds(pl.multiple_of(at * q_rows, q_rows), q_rows), :], load_sem.at[2 + i]))
    loads.append(pltpu.make_async_copy(wd_ref, wd.at[pl.ds(0, hid_loc), :], load_sem.at[6]))
    q_hid = d0.shape[0]
    for i, (piece, at) in enumerate(((d0, quarter), (d1, q_2), (d2, q_1), (d3, q_3))):
        loads.append(pltpu.make_async_copy(piece, wd.at[pl.ds(pl.multiple_of(hid_loc + at * q_hid, q_hid), q_hid), :], load_sem.at[7 + i]))
    loads.append(pltpu.make_async_copy(res_ref, res, load_sem.at[11]))
    for copy in loads:
        copy.start()

    pl.semaphore_wait(barrier, 2)

    def remote(kind, half, src, dst, who):
        return pltpu.make_async_remote_copy(src_ref=src, dst_ref=dst, send_sem=send_sem.at[kind, half], recv_sem=recv_sem.at[kind, half],
                                            device_id={'tp': ids[who]}, device_id_type=pl.DeviceIdType.MESH)

    def part(half):
        return pl.ds(half * blk, blk)

    rows_mate = [remote(0, h, a_ref.at[part(h)], rows.at[1, part(h)], 'mate') for h in range(halves)]
    rows_partner = [remote(1, h, a_ref.at[part(h)], rows.at[2, part(h)], 'partner') for h in range(halves)]
    rows_diag = [remote(2, h, rows.at[2, part(h)], rows.at[3, part(h)], 'mate') for h in range(halves)]
    sum_mate = [remote(3, h, to_mate.at[part(h)], from_mate.at[part(h)], 'mate') for h in range(halves)]
    sum_diag = [remote(4, h, to_diag.at[part(h)], from_diag.at[part(h)], 'mate') for h in range(halves)]
    sum_partner = [remote(5, h, to_partner.at[part(h)], from_partner.at[part(h)], 'partner') for h in range(halves)]
    for h in range(halves):
        rows_partner[h].start()
    for h in range(halves):
        rows_mate[h].start()
    for copy in loads:
        copy.wait()

    near = 2 * halves

    @pl.loop(0, 2 * near)
    def _(step):
        far = step // near
        k = step % near
        slot = (1 - far) * (k // halves) + far * (3 - k % 2)
        half = (1 - far) * (k % halves) + far * (k // 2)
        for h in range(halves):
            @pl.when(step == halves + h)
            def _(h=h):
                rows_mate[h].wait_recv()

            @pl.when(step == near + 2 * h)
            def _(h=h):
                rows_partner[h].wait_recv()
                rows_diag[h].start()
                rows_diag[h].wait_recv()

        at = pl.ds(pl.multiple_of(half * blk, blk), blk)

        @pl.loop(0, 2 * hid_loc // tile)
        def _(j):
            which = j // (hid_loc // tile)
            off = pl.multiple_of(j % (hid_loc // tile) * tile, tile)
            x = jnp.dot(rows[slot, at, :], wu[which, :, pl.ds(off, tile)], preferred_element_type=jnp.float32)
            x = x + bu_ref[which, :, pl.ds(off, tile)]
            cdf = 0.5 * (1.0 + jnp.tanh(math.sqrt(2.0 / math.pi) * (x + 0.044715 * (x * x * x))))
            hid[:, pl.ds(pl.multiple_of(j * tile, tile), tile)] = (x * cdf).astype(hid.dtype)

        @pl.loop(0, width // tile)
        def _(j):
            cols = pl.ds(pl.multiple_of(j * tile, tile), tile)
            stage[:, cols] = jnp.dot(hid[...], wd[:, cols], preferred_element_type=jnp.float32)

        @pl.when(slot == 0)
        def _():
            own[at, :] = stage[...]

        for h in range(halves):
            @pl.when(step == halves + h)
            def _(h=h):
                to_mate[part(h), :] = stage[...].astype(to_mate.dtype)
                sum_mate[h].start()

            @pl.when(step == near + 2 * h)
            def _(h=h):
                to_diag[part(h), :] = stage[...].astype(to_diag.dtype)
                sum_diag[h].start()

            @pl.when(step == near + 2 * h + 1)
            def _(h=h):
                sum_diag[h].wait_recv()
                to_partner[part(h), :] = (stage[...] + from_diag[part(h), :].astype(jnp.float32)).astype(to_partner.dtype)
                sum_partner[h].start()

    for h in range(halves):
        sum_mate[h].wait_recv()
        sum_partner[h].wait_recv()
        total = own[part(h), :] + from_mate[part(h), :].astype(jnp.float32) + from_partner[part(h), :].astype(jnp.float32)
        out_ref[part(h), :] = (res[part(h), :].astype(jnp.float32) + total + bd_ref[...]).astype(out_ref.dtype)
    for copies in (rows_mate, rows_partner, rows_diag, sum_mate, sum_diag, sum_partner):
        for copy in copies:
            copy.wait_send()


def mlp(a, res, w_up, w_down, up_parts, down_parts, bias_up, bias_down, blk=256):
    tok, width = a.shape
    hid_loc = w_up.shape[1]
    any_spec = pl.BlockSpec(memory_space=pl.ANY)
    vmem = pl.BlockSpec(memory_space=pltpu.VMEM)
    bf16, f32 = jnp.bfloat16, jnp.float32
    return pl.pallas_call(
        mlp_kernel,
        out_shape=jax.ShapeDtypeStruct((tok, width), bf16),
        in_specs=[any_spec] * 12 + [vmem, vmem],
        out_specs=vmem,
        scratch_shapes=[
            pltpu.VMEM((2, width, hid_loc), bf16),
            pltpu.VMEM((2 * hid_loc, width), bf16),
            pltpu.VMEM((4, tok, width), bf16),
            pltpu.VMEM((blk, 2 * hid_loc), bf16),
            pltpu.VMEM((blk, width), f32),
            pltpu.VMEM((tok, width), f32),
        ] + [pltpu.VMEM((tok, width), bf16)] * 7 + [
            pltpu.SemaphoreType.DMA((12,)),
            pltpu.SemaphoreType.DMA((6, tok // blk)),
            pltpu.SemaphoreType.DMA((6, tok // blk)),
        ],
        compiler_params=pltpu.CompilerParams(collective_id=0, has_side_effects=True, vmem_limit_bytes=62 << 20),
        cost_estimate=pl.CostEstimate(flops=32 * tok * width * hid_loc, bytes_accessed=8 * width * hid_loc, transcendentals=0),
        name='mlp',
    )(a, res, w_up, w_down, *up_parts, *down_parts, bias_up, bias_down)


def after(value, *events):
    return lax.optimization_barrier((value,) + events)[0]


def solution(mesh):
    tp_size = mesh.shape['tp']

    def local_layer(x_local, prefix_len, k_cache, v_cache, ln1_gain, ln1_bias, w_qkv, b_qkv, w_out, b_out, ln2_gain, ln2_bias, w_up, b_up, w_down, b_down):
        batch_n, tok_loc, width = x_local.shape
        heads_loc, head_dim = k_cache.shape[2], k_cache.shape[3]
        chunk_len = tok_loc * tp_size
        head_ids = lax.axis_index('tp') * heads_loc + jnp.arange(heads_loc)
        slopes = jnp.exp2(-8.0 * (head_ids + 1).astype(jnp.float32) / (heads_loc * tp_size))
        mirror = [(t, tp_size - 2 - 2 * (t // 2) + t % 2) for t in range(tp_size)]
        flips = [[(d, d ^ bit) for d in range(mesh.shape['dp'])] for bit in (1, 2)]
        quarter = lax.axis_index('dp') % 4
        b_up_far = lax.ppermute(b_up, 'tp', mirror)
        bias_up = jnp.stack([b_up, b_up_far])[:, None].astype(jnp.float32)
        normed = layer_norm(x_local, ln1_gain, ln1_bias)
        gathers = []
        for seq in range(batch_n):
            gathers.append(lax.all_gather(normed[seq], 'tp', axis=0, tiled=True))
        k_upd, v_upd, k_heads, v_heads = prep_cache(k_cache, v_cache, normed)

        q_up, q_down = w_up.shape[0] // 4, w_down.shape[0] // 4
        u_0 = lax.ppermute(lax.dynamic_slice_in_dim(w_up, quarter * q_up, q_up), 'tp', mirror)
        d_0 = lax.ppermute(lax.dynamic_slice_in_dim(w_down, quarter * q_down, q_down), 'tp', mirror)
        u_1 = lax.ppermute(u_0, 'dp', flips[0])
        d_1 = lax.ppermute(d_0, 'dp', flips[1])
        u_2 = lax.ppermute(u_0, 'dp', flips[1])
        d_2 = lax.ppermute(d_0, 'dp', flips[0])
        u_3 = lax.ppermute(u_1, 'dp', flips[1])
        d_3 = lax.ppermute(d_1, 'dp', flips[0])
        up_parts, down_parts = (u_0, u_1, u_2, u_3), (d_0, d_1, d_2, d_3)
        rows_new, exchanged = [], []
        zero = jnp.zeros((), jnp.int32)
        early, context = batch_n - 1, None
        for seq in range(batch_n):
            gathered = gathers[seq] if seq == 0 else after(gathers[seq], rows_new[-1][0])
            qkv = (jnp.dot(gathered, w_qkv, preferred_element_type=jnp.float32) + b_qkv.astype(jnp.float32)).astype(jnp.bfloat16)
            where = dict(slots=early, slot=seq, buffer=context) if seq < early else {}
            context, k_new, v_new = attend(seq, prefix_len, slopes, qkv, k_heads, v_heads, owners=tp_size, **where)
            rows_new.append((k_new, v_new))
            if seq >= early - 1:
                exchanged.append(lax.all_to_all(context, 'tp', 0, 0))
        for seq, (k_new, v_new) in enumerate(rows_new):
            at = (jnp.int32(seq), prefix_len[seq], zero, zero)
            new_shape = (1, chunk_len, heads_loc, head_dim)
            k_upd = lax.dynamic_update_slice(k_upd, k_new.reshape(new_shape), at)
            v_upd = lax.dynamic_update_slice(v_upd, v_new.reshape(new_shape), at)
        w_out_all = lax.all_gather(w_out, 'tp', axis=0, tiled=True)
        residual, normed2 = project(*exchanged, x_local, w_out_all, b_out, ln2_gain, ln2_bias)
        tok = batch_n * tok_loc
        x_out = mlp(normed2, residual.reshape(tok, width), w_up, w_down, up_parts, down_parts, bias_up, b_down.astype(jnp.float32)[None])
        return x_out.reshape(batch_n, tok_loc, width), k_upd, v_upd

    tok_spec = P('dp', 'tp', None)
    cache_spec = P('dp', None, 'tp', None)
    replicated = P()
    in_specs = (tok_spec, P('dp'), cache_spec, cache_spec, replicated, replicated, P(None, 'tp'), P('tp'), P('tp', None), replicated, replicated, replicated, P(None, 'tp'), P('tp'), P('tp', None), replicated)
    return jax.shard_map(local_layer, mesh=mesh, in_specs=in_specs, out_specs=(tok_spec, cache_spec, cache_spec), check_vma=False)
```

```python
import functools
import math

import jax
import jax.numpy as jnp
from jax import lax
from jax.experimental import pallas as pl
from jax.experimental.pallas import tpu as pltpu
from jax.sharding import PartitionSpec as P


LN_EPS = 1e-5
LOG2E = math.log2(math.e)
NEG = -1e30


def attn_kernel(seq, q_blk, k_blk, prefix_ref, slope_ref, qkv_ref, k_ref, v_ref, k_raw, v_raw, *rest):
    out_ref, knew_ref, vnew_ref, k_copy, v_copy, acc_ref, m_ref, hold, sem = rest[-9:]
    head = pl.program_id(0)
    qkv_ref = qkv_ref.at[0]
    chunk = qkv_ref.shape[0]
    dim = k_ref.shape[3]
    heads = qkv_ref.shape[1] // (3 * dim)
    start = prefix_ref[seq]
    slope = slope_ref[head] * LOG2E
    scale = dim ** -0.5 * LOG2E

    loads = [pltpu.make_async_copy(src.at[seq], hold.at[i], sem.at[i]) for i, src in enumerate((k_raw, v_raw))]
    stores = [pltpu.make_async_copy(hold.at[i], dst.at[seq], sem.at[2 + i]) for i, dst in enumerate((k_copy, v_copy))]

    @pl.when(head == 0)
    def _():
        for copy in loads:
            copy.start()

    @pl.when(head == heads - 1)
    def _():
        for load, store in zip(loads, stores):
            load.wait()
            store.start()

    def ones(n):
        return (lax.broadcasted_iota(jnp.int32, (n, dim), 1) == 0).astype(jnp.bfloat16)

    def cols(which):
        return pl.ds(pl.multiple_of((3 * head + which) * dim, dim), dim)

    @pl.when(head == 0)
    def _():
        n = 256
        row = lax.broadcasted_iota(jnp.int32, (n, n), 0)
        pick = (row // heads + row % heads * (n // heads) == lax.broadcasted_iota(jnp.int32, (n, n), 1)).astype(jnp.bfloat16)
        for which, dst in ((1, knew_ref), (2, vnew_ref)):
            for i in range(heads * chunk // n):
                rows = pl.ds(i * (n // heads), n // heads)
                both = jnp.concatenate([qkv_ref[rows, (3 * h + which) * dim:(3 * h + which + 1) * dim] for h in range(heads)], axis=0)
                dst[pl.ds(i * n, n), :] = jnp.dot(pick, both, preferred_element_type=jnp.float32).astype(dst.dtype)

    def update(rows, keys, values, bias, masked=None):
        s = lax.dot_general(qkv_ref[rows, cols(0)], keys, (((1,), (1,)), ((), ())), preferred_element_type=jnp.float32)
        s = s * scale + bias
        if masked is not None:
            s = jnp.where(masked, NEG, s)
        m_old = m_ref[rows, :1]
        m_new = jnp.maximum(m_old, jnp.max(s, axis=1, keepdims=True))
        p = jnp.exp2(s - m_new).astype(jnp.bfloat16)
        pv = lax.dot_general(p, jnp.concatenate([values, ones(values.shape[0])], axis=1), (((1,), (0,)), ((), ())), preferred_element_type=jnp.float32)
        acc_ref[rows, :] = acc_ref[rows, :] * jnp.exp2(m_old - m_new) + pv
        m_ref[rows, :] = jnp.broadcast_to(m_new, (q_blk, m_ref.shape[1]))

    col = lax.broadcasted_iota(jnp.int32, (1, k_blk), 1)
    acc_ref[...] = jnp.zeros_like(acc_ref)
    m_ref[...] = jnp.full_like(m_ref, NEG)
    full = start // k_blk

    def prefix_block(i, masked):
        off = pl.multiple_of(i * k_blk, k_blk)
        keys = k_ref[0, 0, pl.ds(off, k_blk), :]
        values = v_ref[0, 0, pl.ds(off, k_blk), :]
        rel = (off + col - start).astype(jnp.float32)
        for r in range(chunk // q_blk):
            update(pl.ds(r * q_blk, q_blk), keys, values, slope * (rel - float(r * q_blk)), (off + col >= start) if masked else None)

    @pl.loop(0, full)
    def _(i):
        prefix_block(i, False)

    @pl.when(full * k_blk < start)
    def _():
        prefix_block(full, True)

    for r in range(chunk // q_blk):
        n = (r + 1) * q_blk
        new_col = lax.broadcasted_iota(jnp.int32, (1, n), 1) - r * q_blk
        bias = slope * new_col.astype(jnp.float32)
        masked = (lax.broadcasted_iota(jnp.int32, (q_blk, n), 1) - r * q_blk) > lax.broadcasted_iota(jnp.int32, (q_blk, n), 0)
        update(pl.ds(r * q_blk, q_blk), qkv_ref[pl.ds(0, n), cols(1)], qkv_ref[pl.ds(0, n), cols(2)], bias, masked)
    total = acc_ref[:, dim:dim + 1]
    out_ref[:, 0] = (acc_ref[:, :dim] / total).astype(out_ref.dtype).reshape(out_ref.shape[0], out_ref.shape[2], dim)

    @pl.when(head == heads - 1)
    def _():
        for store in stores:
            store.wait()


def attend(seq, prefix_len, slopes, qkv, k_heads, v_heads, k_raw, v_raw, copies=(), owners=8, slots=1, slot=0, buffer=None, q_blk=256, k_blk=1024):
    chunk = qkv.shape[1]
    heads, cache_len, dim = k_heads.shape[1:]
    cache_spec = pl.BlockSpec((1, 1, cache_len, dim), lambda h, *_: (seq, h, 0, 0))
    whole = lambda shape: pl.BlockSpec(shape, lambda h, *_: (0, 0))
    rows = jax.ShapeDtypeStruct((heads * chunk, dim), jnp.bfloat16)
    flat = (k_raw.shape[0], cache_len * heads, dim)
    extra = tuple(copies) + (() if buffer is None else (buffer,))
    aliases = {7 + i: 3 + i for i in range(len(copies))} | ({9: 0} if buffer is not None else {})
    any_spec = pl.BlockSpec(memory_space=pl.ANY)
    copied = jax.ShapeDtypeStruct(flat, k_raw.dtype)
    return pl.pallas_call(
        functools.partial(attn_kernel, seq, q_blk, k_blk),
        out_shape=(jax.ShapeDtypeStruct((owners, slots, chunk // owners, heads * dim), jnp.bfloat16), rows, rows, copied, copied),
        grid_spec=pltpu.PrefetchScalarGridSpec(
            num_scalar_prefetch=2,
            grid=(heads,),
            in_specs=[pl.BlockSpec((1,) + qkv.shape[1:], lambda h, *_: (seq, 0, 0)), cache_spec, cache_spec] + [any_spec] * (2 + len(extra)),
            out_specs=(pl.BlockSpec((owners, 1, chunk // owners, dim), lambda h, *_: (0, slot, 0, h)), whole(rows.shape), whole(rows.shape), any_spec, any_spec),
            scratch_shapes=[pltpu.VMEM((chunk, 2 * dim), jnp.float32), pltpu.VMEM((chunk, 128), jnp.float32), pltpu.VMEM((2,) + flat[1:], k_raw.dtype), pltpu.SemaphoreType.DMA((4,))],
        ),
        cost_estimate=pl.CostEstimate(flops=4 * heads * chunk * cache_len * dim, bytes_accessed=4 * heads * cache_len * dim, transcendentals=heads * chunk * cache_len),
        input_output_aliases=aliases,
        name='attend',
    )(prefix_len, slopes, qkv, k_heads, v_heads, k_raw.reshape(flat), v_raw.reshape(flat), *extra)


def split_heads(heads, k_ref, v_ref, k_heads, v_heads):
    n = 256
    per = n // heads
    row = lax.broadcasted_iota(jnp.int32, (n, n), 0)
    pick = (row % per * heads + row // per == lax.broadcasted_iota(jnp.int32, (n, n), 1)).astype(jnp.bfloat16)
    for src, split in ((k_ref, k_heads), (v_ref, v_heads)):
        for i in range(src.shape[1] // n):
            both = jnp.dot(pick, src[0, pl.ds(i * n, n), :], preferred_element_type=jnp.float32).astype(split.dtype)
            for h in range(heads):
                split[0, h, pl.ds(i * per, per), :] = both[h * per:(h + 1) * per]


def gather_kernel(tp_size, heads, x_ref, gain_ref, bias_ref, w_ref, bw_ref, k_ref, v_ref, qkv_ref, k_heads, v_heads,
                  x_in, w_in, rows, q_all, load_sem, out_sem, send_sem, recv_sem):
    me = lax.axis_index('tp')
    ids = {'mate': me + 1 - 2 * (me % 2), 'right': (me + 2) % tp_size, 'left': (me + tp_size - 2) % tp_size}
    batch, tok, _ = x_in.shape
    blk = batch * tok // 2
    seqs = batch // 2

    barrier = pltpu.get_barrier_semaphore()
    for who in ('mate', 'right', 'left'):
        pl.semaphore_signal(barrier, inc=1, device_id={'tp': ids[who]}, device_id_type=pl.DeviceIdType.MESH)
    load_x = pltpu.make_async_copy(x_ref, x_in, load_sem.at[0])
    load_w = pltpu.make_async_copy(w_ref, w_in, load_sem.at[1])
    load_x.start()
    load_w.start()
    load_x.wait()
    n = 64

    @pl.loop(0, batch * tok // n)
    def _(i):
        at = i * n // tok
        off = pl.multiple_of(i * n % tok, n)
        val = x_in[at, pl.ds(off, n), :].astype(jnp.float32)
        centered = val - jnp.mean(val, axis=-1, keepdims=True)
        var = jnp.mean(centered * centered, axis=-1, keepdims=True)
        normed = (centered * lax.rsqrt(var + LN_EPS) * gain_ref[...] + bias_ref[...]).astype(rows.dtype)
        rows[0, i * n // blk, pl.ds(pl.multiple_of(i * n % blk, n), n), :] = normed

    pl.semaphore_wait(barrier, 3)

    def remote(kind, half, src, dst, who):
        return pltpu.make_async_remote_copy(src_ref=rows.at[src, half], dst_ref=rows.at[dst, half], send_sem=send_sem.at[kind, half], recv_sem=recv_sem.at[kind, half],
                                            device_id={'tp': ids[who]}, device_id_type=pl.DeviceIdType.MESH)

    to_right = [remote(0, h, 0, 2, 'right') for h in range(2)]
    to_left = [remote(1, h, 0, 4, 'left') for h in range(2)]
    to_mate = [remote(2 + s, h, 2 * s, 2 * s + 1, 'mate') for s in range(4) for h in range(2)]
    on_right = remote(6, 0, 2, 6, 'right')
    on_left = remote(6, 1, 4, 6, 'left')
    to_right[0].start()
    to_left[1].start()
    to_right[1].start()
    to_left[0].start()
    to_mate[0].start()
    to_mate[1].start()
    load_w.wait()

    flat = k_ref.shape
    part = 2048
    flat_spec = pl.BlockSpec((1, part, flat[2]), lambda b, i: (b, i, 0))
    split_spec = pl.BlockSpec((1, heads, part // heads, flat[2]), lambda b, i: (b, 0, i, 0))
    pltpu.emit_pipeline(
        functools.partial(split_heads, heads),
        grid=(flat[0], flat[1] // part),
        in_specs=[flat_spec, flat_spec],
        out_specs=[split_spec, split_spec],
    )(k_ref, v_ref, k_heads, v_heads)

    order = [(0, 0), (0, 1), (1, 0), (1, 1), (2, 0), (4, 1), (3, 0), (5, 1), (2, 1), (4, 0), (3, 1), (5, 0), (6, 0), (6, 1), (7, 0), (7, 1)]
    outs = []

    def owner(slot):
        chip = (me // 2 + (0, tp_size // 2 - 1, 1, tp_size // 4)[slot // 2]) % (tp_size // 2)
        return 2 * chip + (me % 2 + slot % 2) % 2

    def arrive(slot, half):
        if slot % 2:
            to_mate[slot // 2 * 2 + half].wait_recv()
        elif slot == 2:
            to_right[half].wait_recv()
            if half == 0:
                on_right.start()
            to_mate[2 + half].start()
        elif slot == 4:
            to_left[half].wait_recv()
            if half == 1:
                on_left.start()
            to_mate[4 + half].start()
        elif slot == 6:
            (on_right, on_left)[half].wait_recv()
            to_mate[6 + half].start()

    for slot, half in order[4:6]:
        arrive(slot, half)
    for i, (slot, half) in enumerate(order):
        if not 4 <= i < 6:
            arrive(slot, half)
        who = owner(slot)
        val = jnp.dot(rows[slot, half], w_in[...], preferred_element_type=jnp.float32) + bw_ref[...]
        q_all[slot, half] = val.astype(q_all.dtype)
        for j in range(seqs):
            copy = pltpu.make_async_copy(q_all.at[slot, half, pl.ds(j * tok, tok), :], qkv_ref.at[half * seqs + j, pl.ds(pl.multiple_of(who * tok, tok), tok), :], out_sem.at[i, j])
            copy.start()
            outs.append(copy)
    for copy in outs:
        copy.wait()
    for copy in to_right + to_left + to_mate + [on_right, on_left]:
        copy.wait_send()


def gather_qkv(x, gain, bias, w, bw, k_cache, v_cache, tp_size):
    batch, tok, width = x.shape
    cols = w.shape[1]
    _, length, heads, dim = k_cache.shape
    flat = (batch, length * heads, dim)
    any_spec = pl.BlockSpec(memory_space=pl.ANY)
    vmem = pl.BlockSpec(memory_space=pltpu.VMEM)
    bf16 = jnp.bfloat16
    row = lambda a: a.astype(jnp.float32)[None]
    split_out = jax.ShapeDtypeStruct((batch, heads, length, dim), bf16)
    blk = batch * tok // 2
    return pl.pallas_call(
        functools.partial(gather_kernel, tp_size, heads),
        out_shape=(jax.ShapeDtypeStruct((batch, tok * tp_size, cols), bf16), split_out, split_out),
        in_specs=[any_spec, vmem, vmem, any_spec, vmem, any_spec, any_spec],
        out_specs=(any_spec,) * 3,
        scratch_shapes=[
            pltpu.VMEM((batch, tok, width), bf16),
            pltpu.VMEM((width, cols), bf16),
            pltpu.VMEM((8, 2, blk, width), bf16),
            pltpu.VMEM((8, 2, blk, cols), bf16),
            pltpu.SemaphoreType.DMA((2,)),
            pltpu.SemaphoreType.DMA((16, batch // 2)),
            pltpu.SemaphoreType.DMA((7, 2)),
            pltpu.SemaphoreType.DMA((7, 2)),
        ],
        compiler_params=pltpu.CompilerParams(collective_id=1, has_side_effects=True, vmem_limit_bytes=62 << 20),
        cost_estimate=pl.CostEstimate(flops=2 * batch * tok * tp_size * width * cols, bytes_accessed=8 * batch * length * heads * dim, transcendentals=0),
        name='gather_qkv',
    )(x, row(gain), row(bias), w, row(bw), k_cache.reshape(flat), v_cache.reshape(flat))


def write_kernel(prefix_ref, *refs):
    batch = (len(refs) - 5) // 2
    k_out, v_out, sem = refs[-3:]
    copies = []
    for b in range(batch):
        for which, (src, dst) in enumerate(((refs[b], k_out), (refs[batch + b], v_out))):
            copies.append(pltpu.make_async_copy(src, dst.at[b, pl.ds(prefix_ref[b], src.shape[0])], sem.at[b, which]))
    for copy in copies:
        copy.start()
    for copy in copies:
        copy.wait()


def write_rows(prefix_len, k_new, v_new, k_cache, v_cache):
    batch = len(k_new)
    new_shape = (-1,) + k_cache.shape[2:]
    news = [a.reshape(new_shape) for a in (*k_new, *v_new)]
    any_spec = pl.BlockSpec(memory_space=pl.ANY)
    out = jax.ShapeDtypeStruct(k_cache.shape, k_cache.dtype)
    return pl.pallas_call(
        write_kernel,
        out_shape=(out, out),
        grid_spec=pltpu.PrefetchScalarGridSpec(
            num_scalar_prefetch=1,
            grid=(),
            in_specs=[pl.BlockSpec(memory_space=pltpu.VMEM)] * (2 * batch) + [any_spec, any_spec],
            out_specs=(any_spec, any_spec),
            scratch_shapes=[pltpu.SemaphoreType.DMA((batch, 2))],
        ),
        input_output_aliases={2 * batch + 1: 0, 2 * batch + 2: 1},
        name='write_rows',
    )(prefix_len, *news, k_cache, v_cache)


def proj_kernel(early_ref, late_ref, x_ref, w_ref, b_ref, gain_ref, bias_ref, res_ref, norm_ref, owned, wide):
    step = pl.program_id(0)
    blocks, early, tok, part = early_ref.shape
    batch = x_ref.shape[0]

    @pl.when(step == 0)
    def _():
        for b in range(batch):
            src, at = (early_ref, b) if b < early else (late_ref, b - early)
            for t in range(blocks):
                owned[b * tok:(b + 1) * tok, t * part:(t + 1) * part] = src[t, at]

    tile = w_ref.shape[1]
    total = jnp.dot(owned[...], w_ref[...], preferred_element_type=jnp.float32)
    for b in range(batch):
        row = (x_ref[b].astype(jnp.float32) + total[b * tok:(b + 1) * tok] + b_ref[...]).astype(res_ref.dtype)
        res_ref[b] = row
        wide[b * tok:(b + 1) * tok, pl.ds(pl.multiple_of(step * tile, tile), tile)] = row

    @pl.when(step == pl.num_programs(0) - 1)
    def _():
        n = 64

        @pl.loop(0, wide.shape[0] // n)
        def _(i):
            rows = pl.ds(pl.multiple_of(i * n, n), n)
            val = wide[rows, :].astype(jnp.float32)
            centered = val - jnp.mean(val, axis=-1, keepdims=True)
            var = jnp.mean(centered * centered, axis=-1, keepdims=True)
            norm_ref[rows, :] = (centered * lax.rsqrt(var + LN_EPS) * gain_ref[...] + bias_ref[...]).astype(norm_ref.dtype)


def project(early, late, x, w, b, gain, bias, tile=512):
    batch, tok, width = x.shape
    whole = lambda a: pl.BlockSpec(a.shape, lambda j: (0,) * a.ndim)
    row = lambda a: a.astype(jnp.float32)[None]
    gain, bias = row(gain), row(bias)
    bf16 = jnp.bfloat16
    col = pl.BlockSpec((batch, tok, tile), lambda j: (0, 0, j))
    return pl.pallas_call(
        proj_kernel,
        out_shape=(jax.ShapeDtypeStruct(x.shape, bf16), jax.ShapeDtypeStruct((batch * tok, width), bf16)),
        grid=(width // tile,),
        in_specs=[whole(early), whole(late), col, pl.BlockSpec((width, tile), lambda j: (0, j)), pl.BlockSpec((1, tile), lambda j: (0, j)), whole(gain), whole(bias)],
        out_specs=(col, pl.BlockSpec((batch * tok, width), lambda j: (0, 0))),
        scratch_shapes=[pltpu.VMEM((batch * tok, width), bf16), pltpu.VMEM((batch * tok, width), bf16)],
        cost_estimate=pl.CostEstimate(flops=2 * batch * tok * width * width, bytes_accessed=2 * width * width, transcendentals=0),
        name='project',
    )(early, late, x, w, row(b), gain, bias)


def pair_ids(t):
    return {'mate': t + 1 - 2 * (t % 2), 'partner': t + 2 - 4 * (t // 2 % 2)}


def mlp_kernel(a_ref, res_ref, wu_ref, wd_ref, u0, u1, u2, u3, d0, d1, d2, d3, bu_ref, bd_ref, out_ref,
               wu, wd, rows, hid, stage, own, to_mate, to_diag, to_partner, from_mate, from_diag, from_partner, res,
               load_sem, send_sem, recv_sem):
    me = lax.axis_index('tp')
    ids = pair_ids(me)
    quarter = lax.axis_index('dp') % 4
    q_1 = quarter + 1 - 2 * (quarter % 2)
    q_2 = quarter + 2 - 4 * (quarter // 2)
    q_3 = 3 - quarter
    tok, width = own.shape
    blk = hid.shape[0]
    halves = tok // blk
    hid_loc = wu.shape[2]
    tile = 512

    barrier = pltpu.get_barrier_semaphore()
    for who in ('mate', 'partner'):
        pl.semaphore_signal(barrier, inc=1, device_id={'tp': ids[who]}, device_id_type=pl.DeviceIdType.MESH)

    loads = [pltpu.make_async_copy(a_ref, rows.at[0], load_sem.at[0]), pltpu.make_async_copy(wu_ref, wu.at[0], load_sem.at[1])]
    q_rows = u0.shape[0]
    for i, (piece, at) in enumerate(((u0, quarter), (u1, q_1), (u2, q_2), (u3, q_3))):
        loads.append(pltpu.make_async_copy(piece, wu.at[1, pl.ds(pl.multiple_of(at * q_rows, q_rows), q_rows), :], load_sem.at[2 + i]))
    loads.append(pltpu.make_async_copy(wd_ref, wd.at[pl.ds(0, hid_loc), :], load_sem.at[6]))
    q_hid = d0.shape[0]
    for i, (piece, at) in enumerate(((d0, quarter), (d1, q_2), (d2, q_1), (d3, q_3))):
        loads.append(pltpu.make_async_copy(piece, wd.at[pl.ds(pl.multiple_of(hid_loc + at * q_hid, q_hid), q_hid), :], load_sem.at[7 + i]))
    loads.append(pltpu.make_async_copy(res_ref, res, load_sem.at[11]))
    for copy in loads:
        copy.start()

    pl.semaphore_wait(barrier, 2)

    def remote(kind, half, src, dst, who):
        return pltpu.make_async_remote_copy(src_ref=src, dst_ref=dst, send_sem=send_sem.at[kind, half], recv_sem=recv_sem.at[kind, half],
                                            device_id={'tp': ids[who]}, device_id_type=pl.DeviceIdType.MESH)

    def part(half):
        return pl.ds(half * blk, blk)

    rows_mate = [remote(0, h, a_ref.at[part(h)], rows.at[1, part(h)], 'mate') for h in range(halves)]
    rows_partner = [remote(1, h, a_ref.at[part(h)], rows.at[2, part(h)], 'partner') for h in range(halves)]
    rows_diag = [remote(2, h, rows.at[2, part(h)], rows.at[3, part(h)], 'mate') for h in range(halves)]
    sum_mate = [remote(3, h, to_mate.at[part(h)], from_mate.at[part(h)], 'mate') for h in range(halves)]
    sum_diag = [remote(4, h, to_diag.at[part(h)], from_diag.at[part(h)], 'mate') for h in range(halves)]
    sum_partner = [remote(5, h, to_partner.at[part(h)], from_partner.at[part(h)], 'partner') for h in range(halves)]
    for h in range(halves):
        rows_partner[h].start()
    for h in range(halves):
        rows_mate[h].start()
    for copy in loads:
        copy.wait()

    near = 2 * halves

    @pl.loop(0, 2 * near)
    def _(step):
        far = step // near
        k = step % near
        slot = (1 - far) * (k // halves) + far * (3 - k % 2)
        half = (1 - far) * (k % halves) + far * (k // 2)
        for h in range(halves):
            @pl.when(step == halves + h)
            def _(h=h):
                rows_mate[h].wait_recv()

            @pl.when(step == near + 2 * h)
            def _(h=h):
                rows_partner[h].wait_recv()
                rows_diag[h].start()
                rows_diag[h].wait_recv()

        at = pl.ds(pl.multiple_of(half * blk, blk), blk)

        @pl.loop(0, 2 * hid_loc // tile)
        def _(j):
            which = j // (hid_loc // tile)
            off = pl.multiple_of(j % (hid_loc // tile) * tile, tile)
            x = jnp.dot(rows[slot, at, :], wu[which, :, pl.ds(off, tile)], preferred_element_type=jnp.float32)
            x = x + bu_ref[which, :, pl.ds(off, tile)]
            cdf = 0.5 * (1.0 + jnp.tanh(math.sqrt(2.0 / math.pi) * (x + 0.044715 * (x * x * x))))
            hid[:, pl.ds(pl.multiple_of(j * tile, tile), tile)] = (x * cdf).astype(hid.dtype)

        @pl.loop(0, width // tile)
        def _(j):
            cols = pl.ds(pl.multiple_of(j * tile, tile), tile)
            stage[:, cols] = jnp.dot(hid[...], wd[:, cols], preferred_element_type=jnp.float32)

        @pl.when(slot == 0)
        def _():
            own[at, :] = stage[...]

        for h in range(halves):
            @pl.when(step == halves + h)
            def _(h=h):
                to_mate[part(h), :] = stage[...].astype(to_mate.dtype)
                sum_mate[h].start()

            @pl.when(step == near + 2 * h)
            def _(h=h):
                to_diag[part(h), :] = stage[...].astype(to_diag.dtype)
                sum_diag[h].start()

            @pl.when(step == near + 2 * h + 1)
            def _(h=h):
                sum_diag[h].wait_recv()
                to_partner[part(h), :] = (stage[...] + from_diag[part(h), :].astype(jnp.float32)).astype(to_partner.dtype)
                sum_partner[h].start()

    for h in range(halves):
        sum_mate[h].wait_recv()
        sum_partner[h].wait_recv()
        total = own[part(h), :] + from_mate[part(h), :].astype(jnp.float32) + from_partner[part(h), :].astype(jnp.float32)
        out_ref[part(h), :] = (res[part(h), :].astype(jnp.float32) + total + bd_ref[...]).astype(out_ref.dtype)
    for copies in (rows_mate, rows_partner, rows_diag, sum_mate, sum_diag, sum_partner):
        for copy in copies:
            copy.wait_send()


def mlp(a, res, w_up, w_down, up_parts, down_parts, bias_up, bias_down, blk=256):
    tok, width = a.shape
    hid_loc = w_up.shape[1]
    any_spec = pl.BlockSpec(memory_space=pl.ANY)
    vmem = pl.BlockSpec(memory_space=pltpu.VMEM)
    bf16, f32 = jnp.bfloat16, jnp.float32
    return pl.pallas_call(
        mlp_kernel,
        out_shape=jax.ShapeDtypeStruct((tok, width), bf16),
        in_specs=[any_spec] * 12 + [vmem, vmem],
        out_specs=vmem,
        scratch_shapes=[
            pltpu.VMEM((2, width, hid_loc), bf16),
            pltpu.VMEM((2 * hid_loc, width), bf16),
            pltpu.VMEM((4, tok, width), bf16),
            pltpu.VMEM((blk, 2 * hid_loc), bf16),
            pltpu.VMEM((blk, width), f32),
            pltpu.VMEM((tok, width), f32),
        ] + [pltpu.VMEM((tok, width), bf16)] * 7 + [
            pltpu.SemaphoreType.DMA((12,)),
            pltpu.SemaphoreType.DMA((6, tok // blk)),
            pltpu.SemaphoreType.DMA((6, tok // blk)),
        ],
        compiler_params=pltpu.CompilerParams(collective_id=0, has_side_effects=True, vmem_limit_bytes=62 << 20),
        cost_estimate=pl.CostEstimate(flops=32 * tok * width * hid_loc, bytes_accessed=8 * width * hid_loc, transcendentals=0),
        name='mlp',
    )(a, res, w_up, w_down, *up_parts, *down_parts, bias_up, bias_down)


def solution(mesh):
    tp_size = mesh.shape['tp']

    def local_layer(x_local, prefix_len, k_cache, v_cache, ln1_gain, ln1_bias, w_qkv, b_qkv, w_out, b_out, ln2_gain, ln2_bias, w_up, b_up, w_down, b_down):
        batch_n, tok_loc, width = x_local.shape
        heads_loc = k_cache.shape[2]
        head_ids = lax.axis_index('tp') * heads_loc + jnp.arange(heads_loc)
        slopes = jnp.exp2(-8.0 * (head_ids + 1).astype(jnp.float32) / (heads_loc * tp_size))
        mirror = [(t, tp_size - 2 - 2 * (t // 2) + t % 2) for t in range(tp_size)]
        flips = [[(d, d ^ bit) for d in range(mesh.shape['dp'])] for bit in (1, 2)]
        quarter = lax.axis_index('dp') % 4
        b_up_far = lax.ppermute(b_up, 'tp', mirror)
        bias_up = jnp.stack([b_up, b_up_far])[:, None].astype(jnp.float32)
        qkv, k_heads, v_heads = gather_qkv(x_local, ln1_gain, ln1_bias, w_qkv, b_qkv, k_cache, v_cache, tp_size)

        q_up, q_down = w_up.shape[0] // 4, w_down.shape[0] // 4
        u_0 = lax.ppermute(lax.dynamic_slice_in_dim(w_up, quarter * q_up, q_up), 'tp', mirror)
        d_0 = lax.ppermute(lax.dynamic_slice_in_dim(w_down, quarter * q_down, q_down), 'tp', mirror)
        u_1 = lax.ppermute(u_0, 'dp', flips[0])
        d_1 = lax.ppermute(d_0, 'dp', flips[1])
        u_2 = lax.ppermute(u_0, 'dp', flips[1])
        d_2 = lax.ppermute(d_0, 'dp', flips[0])
        u_3 = lax.ppermute(u_1, 'dp', flips[1])
        d_3 = lax.ppermute(d_1, 'dp', flips[0])
        up_parts, down_parts = (u_0, u_1, u_2, u_3), (d_0, d_1, d_2, d_3)
        rows_new, exchanged = [], []
        early, context, copies = batch_n - 1, None, ()
        for seq in range(batch_n):
            where = dict(slots=early, slot=seq, buffer=context) if seq < early else {}
            context, k_new, v_new, *copies = attend(seq, prefix_len, slopes, qkv, k_heads, v_heads, k_cache, v_cache, copies, owners=tp_size, **where)
            rows_new.append((k_new, v_new))
            if seq >= early - 1:
                exchanged.append(lax.all_to_all(context, 'tp', 0, 0))
        k_upd, v_upd = write_rows(prefix_len, [k for k, _ in rows_new], [v for _, v in rows_new], *(a.reshape(k_cache.shape) for a in copies))
        w_out_all = lax.all_gather(w_out, 'tp', axis=0, tiled=True)
        residual, normed2 = project(*exchanged, x_local, w_out_all, b_out, ln2_gain, ln2_bias)
        tok = batch_n * tok_loc
        x_out = mlp(normed2, residual.reshape(tok, width), w_up, w_down, up_parts, down_parts, bias_up, b_down.astype(jnp.float32)[None])
        return x_out.reshape(batch_n, tok_loc, width), k_upd, v_upd

    tok_spec = P('dp', 'tp', None)
    cache_spec = P('dp', None, 'tp', None)
    replicated = P()
    in_specs = (tok_spec, P('dp'), cache_spec, cache_spec, replicated, replicated, P(None, 'tp'), P('tp'), P('tp', None), replicated, replicated, replicated, P(None, 'tp'), P('tp'), P('tp', None), replicated)
    return jax.shard_map(local_layer, mesh=mesh, in_specs=in_specs, out_specs=(tok_spec, cache_spec, cache_spec), check_vma=False)
```

```python
import functools
import math

import jax
import jax.numpy as jnp
from jax import lax
from jax.experimental import pallas as pl
from jax.experimental.pallas import tpu as pltpu
from jax.sharding import PartitionSpec as P


LN_EPS = 1e-5
LOG2E = math.log2(math.e)
NEG = -1e30


def attn_kernel(seq, q_blk, k_blk, prefix_ref, slope_ref, qkv_ref, k_ref, v_ref, k_raw, v_raw, *rest):
    out_ref, knew_ref, vnew_ref, k_copy, v_copy, acc_ref, m_ref, hold, sem = rest[-9:]
    head = pl.program_id(0)
    qkv_ref = qkv_ref.at[0]
    chunk = qkv_ref.shape[0]
    dim = k_ref.shape[3]
    heads = qkv_ref.shape[1] // (3 * dim)
    start = prefix_ref[seq]
    slope = slope_ref[head] * LOG2E
    scale = dim ** -0.5 * LOG2E

    loads = [pltpu.make_async_copy(src.at[seq], hold.at[i], sem.at[i]) for i, src in enumerate((k_raw, v_raw))]
    stores = [pltpu.make_async_copy(hold.at[i], dst.at[seq], sem.at[2 + i]) for i, dst in enumerate((k_copy, v_copy))]

    @pl.when(head == 0)
    def _():
        for copy in loads:
            copy.start()

    @pl.when(head == heads - 1)
    def _():
        for load, store in zip(loads, stores):
            load.wait()
            store.start()

    def ones(n):
        return (lax.broadcasted_iota(jnp.int32, (n, dim), 1) == 0).astype(jnp.bfloat16)

    def cols(which):
        return pl.ds(pl.multiple_of((3 * head + which) * dim, dim), dim)

    @pl.when(head == 0)
    def _():
        n = 256
        row = lax.broadcasted_iota(jnp.int32, (n, n), 0)
        pick = (row // heads + row % heads * (n // heads) == lax.broadcasted_iota(jnp.int32, (n, n), 1)).astype(jnp.bfloat16)
        for which, dst in ((1, knew_ref), (2, vnew_ref)):
            for i in range(heads * chunk // n):
                rows = pl.ds(i * (n // heads), n // heads)
                both = jnp.concatenate([qkv_ref[rows, (3 * h + which) * dim:(3 * h + which + 1) * dim] for h in range(heads)], axis=0)
                dst[pl.ds(i * n, n), :] = jnp.dot(pick, both, preferred_element_type=jnp.float32).astype(dst.dtype)

    def update(rows, keys, values, bias, masked=None):
        s = lax.dot_general(qkv_ref[rows, cols(0)], keys, (((1,), (1,)), ((), ())), preferred_element_type=jnp.float32)
        s = s * scale + bias
        if masked is not None:
            s = jnp.where(masked, NEG, s)
        m_old = m_ref[rows, :1]
        m_new = jnp.maximum(m_old, jnp.max(s, axis=1, keepdims=True))
        p = jnp.exp2(s - m_new).astype(jnp.bfloat16)
        pv = lax.dot_general(p, jnp.concatenate([values, ones(values.shape[0])], axis=1), (((1,), (0,)), ((), ())), preferred_element_type=jnp.float32)
        acc_ref[rows, :] = acc_ref[rows, :] * jnp.exp2(m_old - m_new) + pv
        m_ref[rows, :] = jnp.broadcast_to(m_new, (q_blk, m_ref.shape[1]))

    col = lax.broadcasted_iota(jnp.int32, (1, k_blk), 1)
    acc_ref[...] = jnp.zeros_like(acc_ref)
    m_ref[...] = jnp.full_like(m_ref, NEG)

    @pl.loop(0, (start + k_blk - 1) // k_blk)
    def _(i):
        off = pl.multiple_of(i * k_blk, k_blk)
        keys = k_ref[0, 0, pl.ds(off, k_blk), :]
        keys = jnp.where(lax.broadcasted_iota(jnp.int32, keys.shape, 0) < start - off, keys, jnp.zeros_like(keys))
        values = v_ref[0, 0, pl.ds(off, k_blk), :]
        rel = (off + col - start).astype(jnp.float32)
        for r in range(chunk // q_blk):
            bias = jnp.where(off + col < start, slope * (rel - float(r * q_blk)), NEG)
            update(pl.ds(r * q_blk, q_blk), keys, values, bias)

    for r in range(chunk // q_blk):
        n = (r + 1) * q_blk
        new_col = lax.broadcasted_iota(jnp.int32, (1, n), 1) - r * q_blk
        bias = slope * new_col.astype(jnp.float32)
        masked = (lax.broadcasted_iota(jnp.int32, (q_blk, n), 1) - r * q_blk) > lax.broadcasted_iota(jnp.int32, (q_blk, n), 0)
        update(pl.ds(r * q_blk, q_blk), qkv_ref[pl.ds(0, n), cols(1)], qkv_ref[pl.ds(0, n), cols(2)], bias, masked)
    total = acc_ref[:, dim:dim + 1]
    out_ref[:, 0] = (acc_ref[:, :dim] / total).astype(out_ref.dtype).reshape(out_ref.shape[0], out_ref.shape[2], dim)

    @pl.when(head == heads - 1)
    def _():
        for store in stores:
            store.wait()


def attend(seq, prefix_len, slopes, qkv, k_heads, v_heads, k_raw, v_raw, copies=(), owners=8, slots=1, slot=0, buffer=None, q_blk=256, k_blk=1024):
    chunk = qkv.shape[1]
    heads, cache_len, dim = k_heads.shape[1:]
    cache_spec = pl.BlockSpec((1, 1, cache_len, dim), lambda h, *_: (seq, h, 0, 0))
    whole = lambda shape: pl.BlockSpec(shape, lambda h, *_: (0, 0))
    rows = jax.ShapeDtypeStruct((heads * chunk, dim), jnp.bfloat16)
    flat = (k_raw.shape[0], cache_len * heads, dim)
    extra = tuple(copies) + (() if buffer is None else (buffer,))
    aliases = {7 + i: 3 + i for i in range(len(copies))} | ({9: 0} if buffer is not None else {})
    any_spec = pl.BlockSpec(memory_space=pl.ANY)
    copied = jax.ShapeDtypeStruct(flat, k_raw.dtype)
    return pl.pallas_call(
        functools.partial(attn_kernel, seq, q_blk, k_blk),
        out_shape=(jax.ShapeDtypeStruct((owners, slots, chunk // owners, heads * dim), jnp.bfloat16), rows, rows, copied, copied),
        grid_spec=pltpu.PrefetchScalarGridSpec(
            num_scalar_prefetch=2,
            grid=(heads,),
            in_specs=[pl.BlockSpec((1,) + qkv.shape[1:], lambda h, *_: (seq, 0, 0)), cache_spec, cache_spec] + [any_spec] * (2 + len(extra)),
            out_specs=(pl.BlockSpec((owners, 1, chunk // owners, dim), lambda h, *_: (0, slot, 0, h)), whole(rows.shape), whole(rows.shape), any_spec, any_spec),
            scratch_shapes=[pltpu.VMEM((chunk, 2 * dim), jnp.float32), pltpu.VMEM((chunk, 128), jnp.float32), pltpu.VMEM((2,) + flat[1:], k_raw.dtype), pltpu.SemaphoreType.DMA((4,))],
        ),
        cost_estimate=pl.CostEstimate(flops=4 * heads * chunk * cache_len * dim, bytes_accessed=4 * heads * cache_len * dim, transcendentals=heads * chunk * cache_len),
        input_output_aliases=aliases,
        name='attend',
    )(prefix_len, slopes, qkv, k_heads, v_heads, k_raw.reshape(flat), v_raw.reshape(flat), *extra)


def split_heads(heads, k_ref, v_ref, k_heads, v_heads):
    n = 256
    per = n // heads
    row = lax.broadcasted_iota(jnp.int32, (n, n), 0)
    pick = (row % per * heads + row // per == lax.broadcasted_iota(jnp.int32, (n, n), 1)).astype(jnp.bfloat16)
    for src, split in ((k_ref, k_heads), (v_ref, v_heads)):
        for i in range(src.shape[1] // n):
            both = jnp.dot(pick, src[0, pl.ds(i * n, n), :], preferred_element_type=jnp.float32).astype(split.dtype)
            for h in range(heads):
                split[0, h, pl.ds(i * per, per), :] = both[h * per:(h + 1) * per]


def gather_kernel(tp_size, heads, x_ref, gain_ref, bias_ref, w_ref, bw_ref, k_ref, v_ref, qkv_ref, k_heads, v_heads,
                  x_in, w_in, rows, q_all, load_sem, out_sem, send_sem, recv_sem):
    me = lax.axis_index('tp')
    ids = {'mate': me + 1 - 2 * (me % 2), 'right': (me + 2) % tp_size, 'left': (me + tp_size - 2) % tp_size}
    batch, tok, _ = x_in.shape
    blk = batch * tok // 2
    seqs = batch // 2

    barrier = pltpu.get_barrier_semaphore()
    for who in ('mate', 'right', 'left'):
        pl.semaphore_signal(barrier, inc=1, device_id={'tp': ids[who]}, device_id_type=pl.DeviceIdType.MESH)
    load_x = pltpu.make_async_copy(x_ref, x_in, load_sem.at[0])
    load_w = pltpu.make_async_copy(w_ref, w_in, load_sem.at[1])
    load_x.start()
    load_w.start()
    load_x.wait()
    n = 128

    @pl.loop(0, batch * tok // n)
    def _(i):
        at = i * n // tok
        off = pl.multiple_of(i * n % tok, n)
        val = x_in[at, pl.ds(off, n), :].astype(jnp.float32)
        centered = val - jnp.mean(val, axis=-1, keepdims=True)
        var = jnp.mean(centered * centered, axis=-1, keepdims=True)
        normed = (centered * lax.rsqrt(var + LN_EPS) * gain_ref[...].astype(jnp.float32)[None] + bias_ref[...].astype(jnp.float32)[None]).astype(rows.dtype)
        rows[0, i * n // blk, pl.ds(pl.multiple_of(i * n % blk, n), n), :] = normed

    pl.semaphore_wait(barrier, 3)

    def remote(kind, half, src, dst, who):
        return pltpu.make_async_remote_copy(src_ref=rows.at[src, half], dst_ref=rows.at[dst, half], send_sem=send_sem.at[kind, half], recv_sem=recv_sem.at[kind, half],
                                            device_id={'tp': ids[who]}, device_id_type=pl.DeviceIdType.MESH)

    to_right = [remote(0, h, 0, 2, 'right') for h in range(2)]
    to_left = [remote(1, h, 0, 4, 'left') for h in range(2)]
    to_mate = [remote(2 + s, h, 2 * s, 2 * s + 1, 'mate') for s in range(4) for h in range(2)]
    on_right = remote(6, 0, 2, 6, 'right')
    on_left = remote(6, 1, 4, 6, 'left')
    to_right[0].start()
    to_left[1].start()
    to_right[1].start()
    to_left[0].start()
    to_mate[0].start()
    to_mate[1].start()
    load_w.wait()

    flat = k_ref.shape
    part = 2048
    flat_spec = pl.BlockSpec((1, part, flat[2]), lambda b, i: (b, i, 0))
    split_spec = pl.BlockSpec((1, heads, part // heads, flat[2]), lambda b, i: (b, 0, i, 0))
    pltpu.emit_pipeline(
        functools.partial(split_heads, heads),
        grid=(flat[0], flat[1] // part),
        in_specs=[flat_spec, flat_spec],
        out_specs=[split_spec, split_spec],
    )(k_ref, v_ref, k_heads, v_heads)

    order = [(0, 0), (0, 1), (1, 0), (1, 1), (2, 0), (4, 1), (3, 0), (5, 1), (2, 1), (4, 0), (3, 1), (5, 0), (6, 0), (6, 1), (7, 0), (7, 1)]

    def arrive(slot, half):
        if slot % 2:
            to_mate[slot // 2 * 2 + half].wait_recv()
        elif slot == 2:
            to_right[half].wait_recv()
            if half == 0:
                on_right.start()
            to_mate[2 + half].start()
        elif slot == 4:
            to_left[half].wait_recv()
            if half == 1:
                on_left.start()
            to_mate[4 + half].start()
        elif slot == 6:
            (on_right, on_left)[half].wait_recv()
            to_mate[6 + half].start()

    for slot, half in order[4:6]:
        arrive(slot, half)

    def pick(i, values):
        return sum((v * (i == j).astype(jnp.int32) for j, v in enumerate(values) if v), jnp.int32(0))

    def out_copy(i, j):
        slot = pick(i, [s for s, _ in order])
        half = pick(i, [h for _, h in order])
        chips = tp_size // 2
        chip = (me // 2 + pick(slot // 2, (0, chips - 1, 1, chips // 2))) % chips
        who = 2 * chip + (me % 2 + slot % 2) % 2
        return pltpu.make_async_copy(q_all.at[slot, half, pl.ds(j * tok, tok), :], qkv_ref.at[half * seqs + j, pl.ds(pl.multiple_of(who * tok, tok), tok), :], out_sem.at[i, j])

    @pl.loop(0, len(order))
    def _(i):
        for k, (slot, half) in enumerate(order):
            if not 4 <= k < 6:
                @pl.when(i == k)
                def _(slot=slot, half=half):
                    arrive(slot, half)
        slot = pick(i, [s for s, _ in order])
        half = pick(i, [h for _, h in order])
        val = jnp.dot(rows[slot, half], w_in[...], preferred_element_type=jnp.float32) + bw_ref[...].astype(jnp.float32)[None]
        q_all[slot, half] = val.astype(q_all.dtype)
        for j in range(seqs):
            out_copy(i, j).start()

    @pl.loop(0, len(order))
    def _(i):
        for j in range(seqs):
            out_copy(i, j).wait()

    for copy in to_right + to_left + to_mate + [on_right, on_left]:
        copy.wait_send()


def gather_qkv(x, gain, bias, w, bw, k_cache, v_cache, tp_size):
    batch, tok, width = x.shape
    cols = w.shape[1]
    _, length, heads, dim = k_cache.shape
    flat = (batch, length * heads, dim)
    any_spec = pl.BlockSpec(memory_space=pl.ANY)
    vmem = pl.BlockSpec(memory_space=pltpu.VMEM)
    bf16 = jnp.bfloat16
    split_out = jax.ShapeDtypeStruct((batch, heads, length, dim), bf16)
    blk = batch * tok // 2
    return pl.pallas_call(
        functools.partial(gather_kernel, tp_size, heads),
        out_shape=(jax.ShapeDtypeStruct((batch, tok * tp_size, cols), bf16), split_out, split_out),
        in_specs=[any_spec, vmem, vmem, any_spec, vmem, any_spec, any_spec],
        out_specs=(any_spec,) * 3,
        scratch_shapes=[
            pltpu.VMEM((batch, tok, width), bf16),
            pltpu.VMEM((width, cols), bf16),
            pltpu.VMEM((8, 2, blk, width), bf16),
            pltpu.VMEM((8, 2, blk, cols), bf16),
            pltpu.SemaphoreType.DMA((2,)),
            pltpu.SemaphoreType.DMA((16, batch // 2)),
            pltpu.SemaphoreType.DMA((7, 2)),
            pltpu.SemaphoreType.DMA((7, 2)),
        ],
        compiler_params=pltpu.CompilerParams(collective_id=1, has_side_effects=True, vmem_limit_bytes=62 << 20),
        cost_estimate=pl.CostEstimate(flops=2 * batch * tok * tp_size * width * cols, bytes_accessed=8 * batch * length * heads * dim, transcendentals=0),
        name='gather_qkv',
    )(x, gain, bias, w, bw, k_cache.reshape(flat), v_cache.reshape(flat))


def write_kernel(prefix_ref, *refs):
    batch = (len(refs) - 5) // 2
    k_out, v_out, sem = refs[-3:]
    copies = []
    for b in range(batch):
        for which, (src, dst) in enumerate(((refs[b], k_out), (refs[batch + b], v_out))):
            copies.append(pltpu.make_async_copy(src, dst.at[b, pl.ds(prefix_ref[b], src.shape[0])], sem.at[b, which]))
    for copy in copies:
        copy.start()
    for copy in copies:
        copy.wait()


def write_rows(prefix_len, k_new, v_new, k_cache, v_cache):
    batch = len(k_new)
    new_shape = (-1,) + k_cache.shape[2:]
    news = [a.reshape(new_shape) for a in (*k_new, *v_new)]
    any_spec = pl.BlockSpec(memory_space=pl.ANY)
    out = jax.ShapeDtypeStruct(k_cache.shape, k_cache.dtype)
    return pl.pallas_call(
        write_kernel,
        out_shape=(out, out),
        grid_spec=pltpu.PrefetchScalarGridSpec(
            num_scalar_prefetch=1,
            grid=(),
            in_specs=[pl.BlockSpec(memory_space=pltpu.VMEM)] * (2 * batch) + [any_spec, any_spec],
            out_specs=(any_spec, any_spec),
            scratch_shapes=[pltpu.SemaphoreType.DMA((batch, 2))],
        ),
        input_output_aliases={2 * batch + 1: 0, 2 * batch + 2: 1},
        name='write_rows',
    )(prefix_len, *news, k_cache, v_cache)


def proj_kernel(early_ref, late_ref, x_ref, w_ref, b_ref, gain_ref, bias_ref, res_ref, norm_ref, owned, wide):
    step = pl.program_id(0)
    blocks, early, tok, part = early_ref.shape
    batch = x_ref.shape[0]

    @pl.when(step == 0)
    def _():
        for b in range(batch):
            src, at = (early_ref, b) if b < early else (late_ref, b - early)
            for t in range(blocks):
                owned[b * tok:(b + 1) * tok, t * part:(t + 1) * part] = src[t, at]

    tile = w_ref.shape[1]
    total = jnp.dot(owned[...], w_ref[...], preferred_element_type=jnp.float32)
    for b in range(batch):
        row = (x_ref[b].astype(jnp.float32) + total[b * tok:(b + 1) * tok] + b_ref[...].astype(jnp.float32)[None]).astype(res_ref.dtype)
        res_ref[b] = row
        wide[b * tok:(b + 1) * tok, pl.ds(pl.multiple_of(step * tile, tile), tile)] = row

    @pl.when(step == pl.num_programs(0) - 1)
    def _():
        n = 128

        @pl.loop(0, wide.shape[0] // n)
        def _(i):
            rows = pl.ds(pl.multiple_of(i * n, n), n)
            val = wide[rows, :].astype(jnp.float32)
            centered = val - jnp.mean(val, axis=-1, keepdims=True)
            var = jnp.mean(centered * centered, axis=-1, keepdims=True)
            norm_ref[rows, :] = (centered * lax.rsqrt(var + LN_EPS) * gain_ref[...].astype(jnp.float32)[None] + bias_ref[...].astype(jnp.float32)[None]).astype(norm_ref.dtype)


def project(early, late, x, w, b, gain, bias, tile=512):
    batch, tok, width = x.shape
    whole = lambda a: pl.BlockSpec(a.shape, lambda j: (0,) * a.ndim)
    bf16 = jnp.bfloat16
    col = pl.BlockSpec((batch, tok, tile), lambda j: (0, 0, j))
    return pl.pallas_call(
        proj_kernel,
        out_shape=(jax.ShapeDtypeStruct(x.shape, bf16), jax.ShapeDtypeStruct((batch * tok, width), bf16)),
        grid=(width // tile,),
        in_specs=[whole(early), whole(late), col, pl.BlockSpec((width, tile), lambda j: (0, j)), pl.BlockSpec((tile,), lambda j: (j,)), whole(gain), whole(bias)],
        out_specs=(col, pl.BlockSpec((batch * tok, width), lambda j: (0, 0))),
        scratch_shapes=[pltpu.VMEM((batch * tok, width), bf16), pltpu.VMEM((batch * tok, width), bf16)],
        cost_estimate=pl.CostEstimate(flops=2 * batch * tok * width * width, bytes_accessed=2 * width * width, transcendentals=0),
        name='project',
    )(early, late, x, w, b, gain, bias)


def pair_ids(t):
    return {'mate': t + 1 - 2 * (t % 2), 'partner': t + 2 - 4 * (t // 2 % 2)}


def mlp_kernel(a_ref, res_ref, wu_ref, wd_ref, u0, u1, u2, u3, d0, d1, d2, d3, bu_ref, bd_ref, out_ref,
               wu, wd, rows, hid, stage, own, to_mate, to_diag, to_partner, from_mate, from_diag, from_partner, res, bias_far, bias,
               load_sem, send_sem, recv_sem):
    me = lax.axis_index('tp')
    ids = pair_ids(me)
    quarter = lax.axis_index('dp') % 4
    q_1 = quarter + 1 - 2 * (quarter % 2)
    q_2 = quarter + 2 - 4 * (quarter // 2)
    q_3 = 3 - quarter
    tok, width = own.shape
    blk = hid.shape[0]
    halves = tok // blk
    hid_loc = wu.shape[2]
    tile = 512

    barrier = pltpu.get_barrier_semaphore()
    for who in ('mate', 'partner'):
        pl.semaphore_signal(barrier, inc=1, device_id={'tp': ids[who]}, device_id_type=pl.DeviceIdType.MESH)

    loads = [pltpu.make_async_copy(a_ref, rows.at[0], load_sem.at[0]), pltpu.make_async_copy(wu_ref, wu.at[0], load_sem.at[1])]
    q_rows = wu.shape[1] // 4
    for i, (piece, at) in enumerate(((u0, quarter), (u1, q_1), (u2, q_2), (u3, q_3))):
        loads.append(pltpu.make_async_copy(piece.at[pl.ds(0, q_rows)], wu.at[1, pl.ds(pl.multiple_of(at * q_rows, q_rows), q_rows), :], load_sem.at[2 + i]))
    loads.append(pltpu.make_async_copy(wd_ref, wd.at[pl.ds(0, hid_loc), :], load_sem.at[6]))
    q_hid = d0.shape[0]
    for i, (piece, at) in enumerate(((d0, quarter), (d1, q_2), (d2, q_1), (d3, q_3))):
        loads.append(pltpu.make_async_copy(piece, wd.at[pl.ds(pl.multiple_of(hid_loc + at * q_hid, q_hid), q_hid), :], load_sem.at[7 + i]))
    loads.append(pltpu.make_async_copy(res_ref, res, load_sem.at[11]))
    loads.append(pltpu.make_async_copy(u0.at[pl.ds(q_rows, bias_far.shape[0])], bias_far, load_sem.at[12]))
    for copy in loads:
        copy.start()

    pl.semaphore_wait(barrier, 2)

    def remote(kind, half, src, dst, who):
        return pltpu.make_async_remote_copy(src_ref=src, dst_ref=dst, send_sem=send_sem.at[kind, half], recv_sem=recv_sem.at[kind, half],
                                            device_id={'tp': ids[who]}, device_id_type=pl.DeviceIdType.MESH)

    def part(half):
        return pl.ds(half * blk, blk)

    rows_mate = [remote(0, h, a_ref.at[part(h)], rows.at[1, part(h)], 'mate') for h in range(halves)]
    rows_partner = [remote(1, h, a_ref.at[part(h)], rows.at[2, part(h)], 'partner') for h in range(halves)]
    rows_diag = [remote(2, h, rows.at[2, part(h)], rows.at[3, part(h)], 'mate') for h in range(halves)]
    sum_mate = [remote(3, h, to_mate.at[part(h)], from_mate.at[part(h)], 'mate') for h in range(halves)]
    sum_diag = [remote(4, h, to_diag.at[part(h)], from_diag.at[part(h)], 'mate') for h in range(halves)]
    sum_partner = [remote(5, h, to_partner.at[part(h)], from_partner.at[part(h)], 'partner') for h in range(halves)]
    for h in range(halves):
        rows_partner[h].start()
    for h in range(halves):
        rows_mate[h].start()
    for copy in loads:
        copy.wait()
    bias[0] = bu_ref[...].astype(jnp.float32)[None]
    bias[1] = bias_far[...].astype(jnp.float32)[:1]

    near = 2 * halves

    @pl.loop(0, 2 * near)
    def _(step):
        far = step // near
        k = step % near
        slot = (1 - far) * (k // halves) + far * (3 - k % 2)
        half = (1 - far) * (k % halves) + far * (k // 2)
        for h in range(halves):
            @pl.when(step == halves + h)
            def _(h=h):
                rows_mate[h].wait_recv()

            @pl.when(step == near + 2 * h)
            def _(h=h):
                rows_partner[h].wait_recv()
                rows_diag[h].start()
                rows_diag[h].wait_recv()

        at = pl.ds(pl.multiple_of(half * blk, blk), blk)

        @pl.loop(0, 2 * hid_loc // tile)
        def _(j):
            which = j // (hid_loc // tile)
            off = pl.multiple_of(j % (hid_loc // tile) * tile, tile)
            x = jnp.dot(rows[slot, at, :], wu[which, :, pl.ds(off, tile)], preferred_element_type=jnp.float32)
            x = x + bias[which, :, pl.ds(off, tile)]
            cdf = 0.5 * (1.0 + jnp.tanh(math.sqrt(2.0 / math.pi) * (x + 0.044715 * (x * x * x))))
            hid[:, pl.ds(pl.multiple_of(j * tile, tile), tile)] = (x * cdf).astype(hid.dtype)

        @pl.loop(0, width // tile)
        def _(j):
            cols = pl.ds(pl.multiple_of(j * tile, tile), tile)
            stage[:, cols] = jnp.dot(hid[...], wd[:, cols], preferred_element_type=jnp.float32)

        @pl.when(slot == 0)
        def _():
            own[at, :] = stage[...]

        for h in range(halves):
            @pl.when(step == halves + h)
            def _(h=h):
                to_mate[part(h), :] = stage[...].astype(to_mate.dtype)
                sum_mate[h].start()

            @pl.when(step == near + 2 * h)
            def _(h=h):
                to_diag[part(h), :] = stage[...].astype(to_diag.dtype)
                sum_diag[h].start()

            @pl.when(step == near + 2 * h + 1)
            def _(h=h):
                sum_diag[h].wait_recv()
                to_partner[part(h), :] = (stage[...] + from_diag[part(h), :].astype(jnp.float32)).astype(to_partner.dtype)
                sum_partner[h].start()

    for h in range(halves):
        sum_mate[h].wait_recv()
        sum_partner[h].wait_recv()
        total = own[part(h), :] + from_mate[part(h), :].astype(jnp.float32) + from_partner[part(h), :].astype(jnp.float32)
        out_ref[part(h), :] = (res[part(h), :].astype(jnp.float32) + total + bd_ref[...].astype(jnp.float32)[None]).astype(out_ref.dtype)
    for copies in (rows_mate, rows_partner, rows_diag, sum_mate, sum_diag, sum_partner):
        for copy in copies:
            copy.wait_send()


def mlp(a, res, w_up, w_down, up_parts, down_parts, bias_up, bias_down, blk=256):
    tok, width = a.shape
    hid_loc = w_up.shape[1]
    any_spec = pl.BlockSpec(memory_space=pl.ANY)
    vmem = pl.BlockSpec(memory_space=pltpu.VMEM)
    bf16, f32 = jnp.bfloat16, jnp.float32
    return pl.pallas_call(
        mlp_kernel,
        out_shape=jax.ShapeDtypeStruct((tok, width), bf16),
        in_specs=[any_spec] * 12 + [vmem, vmem],
        out_specs=vmem,
        scratch_shapes=[
            pltpu.VMEM((2, width, hid_loc), bf16),
            pltpu.VMEM((2 * hid_loc, width), bf16),
            pltpu.VMEM((4, tok, width), bf16),
            pltpu.VMEM((blk, 2 * hid_loc), bf16),
            pltpu.VMEM((blk, width), f32),
            pltpu.VMEM((tok, width), f32),
        ] + [pltpu.VMEM((tok, width), bf16)] * 7 + [
            pltpu.VMEM((16, hid_loc), bf16),
            pltpu.VMEM((2, 1, hid_loc), f32),
            pltpu.SemaphoreType.DMA((13,)),
            pltpu.SemaphoreType.DMA((6, tok // blk)),
            pltpu.SemaphoreType.DMA((6, tok // blk)),
        ],
        compiler_params=pltpu.CompilerParams(collective_id=0, has_side_effects=True, vmem_limit_bytes=62 << 20),
        cost_estimate=pl.CostEstimate(flops=32 * tok * width * hid_loc, bytes_accessed=8 * width * hid_loc, transcendentals=0),
        name='mlp',
    )(a, res, w_up, w_down, *up_parts, *down_parts, bias_up, bias_down)


def solution(mesh):
    tp_size = mesh.shape['tp']

    def local_layer(x_local, prefix_len, k_cache, v_cache, ln1_gain, ln1_bias, w_qkv, b_qkv, w_out, b_out, ln2_gain, ln2_bias, w_up, b_up, w_down, b_down):
        batch_n, tok_loc, width = x_local.shape
        heads_loc = k_cache.shape[2]
        head_ids = lax.axis_index('tp') * heads_loc + jnp.arange(heads_loc)
        slopes = jnp.exp2(-8.0 * (head_ids + 1).astype(jnp.float32) / (heads_loc * tp_size))
        mirror = [(t, tp_size - 2 - 2 * (t // 2) + t % 2) for t in range(tp_size)]
        flips = [[(d, d ^ bit) for d in range(mesh.shape['dp'])] for bit in (1, 2)]
        quarter = lax.axis_index('dp') % 4
        qkv, k_heads, v_heads = gather_qkv(x_local, ln1_gain, ln1_bias, w_qkv, b_qkv, k_cache, v_cache, tp_size)

        q_up, q_down = w_up.shape[0] // 4, w_down.shape[0] // 4
        quarter_up = lax.dynamic_slice_in_dim(w_up, quarter * q_up, q_up)
        bias_rows = jnp.broadcast_to(b_up[None], (16, b_up.shape[0]))
        u_0 = lax.ppermute(jnp.concatenate([quarter_up, bias_rows]), 'tp', mirror)
        d_0 = lax.ppermute(lax.dynamic_slice_in_dim(w_down, quarter * q_down, q_down), 'tp', mirror)
        u_1 = lax.ppermute(u_0, 'dp', flips[0])
        d_1 = lax.ppermute(d_0, 'dp', flips[1])
        u_2 = lax.ppermute(u_0, 'dp', flips[1])
        d_2 = lax.ppermute(d_0, 'dp', flips[0])
        u_3 = lax.ppermute(u_1, 'dp', flips[1])
        d_3 = lax.ppermute(d_1, 'dp', flips[0])
        up_parts, down_parts = (u_0, u_1, u_2, u_3), (d_0, d_1, d_2, d_3)
        rows_new, exchanged = [], []
        early, context, copies = batch_n - 1, None, ()
        for seq in range(batch_n):
            where = dict(slots=early, slot=seq, buffer=context) if seq < early else {}
            context, k_new, v_new, *copies = attend(seq, prefix_len, slopes, qkv, k_heads, v_heads, k_cache, v_cache, copies, owners=tp_size, **where)
            rows_new.append((k_new, v_new))
            if seq >= early - 1:
                exchanged.append(lax.all_to_all(context, 'tp', 0, 0))
        k_upd, v_upd = write_rows(prefix_len, [k for k, _ in rows_new], [v for _, v in rows_new], *(a.reshape(k_cache.shape) for a in copies))
        w_out_all = lax.all_gather(w_out, 'tp', axis=0, tiled=True)
        residual, normed2 = project(*exchanged, x_local, w_out_all, b_out, ln2_gain, ln2_bias)
        tok = batch_n * tok_loc
        x_out = mlp(normed2, residual.reshape(tok, width), w_up, w_down, up_parts, down_parts, b_up, b_down)
        return x_out.reshape(batch_n, tok_loc, width), k_upd, v_upd

    tok_spec = P('dp', 'tp', None)
    cache_spec = P('dp', None, 'tp', None)
    replicated = P()
    in_specs = (tok_spec, P('dp'), cache_spec, cache_spec, replicated, replicated, P(None, 'tp'), P('tp'), P('tp', None), replicated, replicated, replicated, P(None, 'tp'), P('tp'), P('tp', None), replicated)
    return jax.shard_map(local_layer, mesh=mesh, in_specs=in_specs, out_specs=(tok_spec, cache_spec, cache_spec), check_vma=False)
```
